32 devices in a mesh: gene: 4 (over z), var: 4 (over y, core), perm: 2 (over x).
Axes of the slice: x: 2, y: 2, z: 4, core: 2. Of those that a mesh axis runs over, the one named last changes fastest.
Arguments:
- genotypes: bfloat16 [4, 6144, 768], P('gene', ('var', 'perm')), may hold values from 0 to 2
- phenotypes: float32 [512, 768], P('gene'), may hold values from -6 to 6
- perm_rows: int32 [256, 768], P(('var', 'perm')), may hold values from 0 to 767, each once within a row
- starts: int32 [512], P('gene'), may hold values from 0 to 2048, as said below
Outputs:
- maxima: float32 [256, 512], P(('var', 'perm'), 'gene')
- moments: float32 [2, 512], P(None, 'gene')
- pooled: float32 [2], replicated
The draws below stay inside these ranges and needn't reach their ends.
Inputs may be any that keep to these rules, and one draw needn't show every extreme that they name: `perm_rows`: each row is a permutation of 0 to 767. Within each block of 128 genes the starts never fall; a gene's window of 4096 variants lies inside its block's 6144 variants.
All inputs are finite; a program needn't handle non-finite values.
Results may differ from the reference program's by a relative error of at most 0.0023.
Values may be sent and summed in bfloat16 or wider, within the bound.
A program may use at most 64 MiB of HBM per device.

```python
import math
import jax
import jax.numpy as jnp
from jax import lax

SAMPLES = 768
WINDOW = 4096
SPAN = 6144
PERMS = 256
BLOCK_GENES = 128
BLOCKS = 4
GENES = 512


def draw_starts(key, part):
    drawn = jax.random.randint(key, (GENES,), 0, SPAN - WINDOW + 1, dtype=jnp.int32)
    return jnp.sort(drawn.reshape(GENES // BLOCK_GENES, BLOCK_GENES), axis=1).reshape(GENES)


def draw_genotypes(key, part):
    order_key = jax.random.fold_in(key, 11)
    shared_key = jax.random.fold_in(key, 12)
    own_key = jax.random.fold_in(key, 13)
    ranks = jax.random.permutation(order_key, BLOCKS).astype(jnp.float32)
    weights = 0.8 * ranks / max(BLOCKS - 1, 1)
    shared = jax.random.uniform(shared_key, (BLOCKS, 1, SAMPLES), dtype=jnp.float32, minval=0.0, maxval=2.0)
    own = jax.random.uniform(own_key, (BLOCKS, SPAN, SAMPLES), dtype=jnp.float32, minval=0.0, maxval=2.0)
    mixed = weights[:, None, None] * shared + (1.0 - weights[:, None, None]) * own
    return mixed.astype(jnp.bfloat16)


def steps_of(stream_key, dims, split, least, top_value):
    level, own = 1.0, jax.random.fold_in(stream_key, 6)
    for axis_at, shards_of in split:
        draws = jnp.exp(jax.random.uniform(jax.random.fold_in(own, axis_at), (shards_of,), jnp.float32, least / len(split), top_value / len(split)))
        level = level * jnp.repeat(draws, dims[axis_at] // shards_of).reshape([-1 if axis == axis_at else 1 for axis in range(len(dims))])
    return level


def bell_draw(key, dims, spread, limit, split=(), kind=jnp.bfloat16):
    values = spread * jax.random.normal(key, dims, jnp.float32)
    if split:
        values = values * steps_of(key, dims, split, -0.22, 0.18)
    return jnp.clip(values, -limit, limit).astype(kind)


def setup_inputs(seed: int = 0) -> dict:
    keys = jax.random.split(jax.random.key(seed), 5)
    return {
        "genotypes": draw_genotypes(jax.random.fold_in(keys[4], 71), 0),
        "phenotypes": bell_draw(keys[1], (GENES, SAMPLES), 1.0, 6.0, ((0, 4),), jnp.float32),
        "perm_rows": jax.vmap(lambda own: jax.random.permutation(own, SAMPLES))(jax.random.split(keys[2], PERMS)).reshape((PERMS, SAMPLES)).astype(jnp.int32),
        "starts": draw_starts(jax.random.fold_in(keys[4], 71), 0),
    }


def standard_rows(values):
    as_float = values.astype(jnp.float32)
    centred = as_float - lax.optimization_barrier(jnp.mean(as_float, axis=1, keepdims=True))
    inv_norm = lax.rsqrt(lax.optimization_barrier(jnp.sum(centred * centred, axis=1, keepdims=True)) + 1.0)
    return (centred * inv_norm).astype(jnp.bfloat16)

def reference(genotypes, phenotypes, perm_rows, starts):
    blocks = genotypes.shape[0]
    region = genotypes.shape[1]
    samples = phenotypes.shape[1]
    block_genes = phenotypes.shape[0] // blocks
    geno_std = jax.vmap(standard_rows)(genotypes)
    pheno_std = standard_rows(phenotypes).reshape(blocks, block_genes, samples)
    start_rows = starts.reshape(blocks, block_genes)
    positions = jnp.arange(region, dtype=jnp.int32)[None, :, None]
    in_window = (positions >= start_rows[:, None, :]) & (positions < start_rows[:, None, :] + WINDOW)
    perm_block = math.gcd(perm_rows.shape[0], 16)

    def per_perms(index_rows):

        def per_block(operands):
            rows_std, genes_std, window_mask = operands
            perm_table = jnp.take(genes_std.T, index_rows, axis=0)
            scores = jnp.einsum('vs,psg->vpg', rows_std.astype(jnp.float32), perm_table.astype(jnp.float32))
            return lax.optimization_barrier(jnp.max(jnp.where(window_mask[:, None, :], scores * scores, 0.0), axis=0))
        return lax.map(per_block, (geno_std, pheno_std, in_window))
    best_sq = lax.map(per_perms, perm_rows.reshape(-1, perm_block, samples))
    maxima = jnp.transpose(best_sq, (0, 2, 1, 3)).reshape(perm_rows.shape[0], blocks * block_genes) * samples
    log_stat = jnp.log1p(maxima)
    moments = jnp.stack((lax.optimization_barrier(jnp.sum(log_stat, axis=0)), lax.optimization_barrier(jnp.sum(log_stat * log_stat, axis=0)))) / perm_rows.shape[0]
    pooled = lax.optimization_barrier(jnp.sum(moments, axis=1)) / moments.shape[1]
    return (maxima, moments, pooled)
```

```python
import functools

import jax
import jax.numpy as jnp
from jax import lax
from jax.experimental import pallas as pl
from jax.experimental.pallas import tpu as pltpu
from jax.sharding import PartitionSpec as P

WINDOW = 4096
MESH = pl.DeviceIdType.MESH
UNROLL = 8


def standard_rows(values):
    as_float = values.astype(jnp.float32)
    centred = as_float - jnp.mean(as_float, axis=1, keepdims=True)
    inv_norm = lax.rsqrt(jnp.sum(centred * centred, axis=1, keepdims=True) + 1.0)
    return (centred * inv_norm).astype(jnp.bfloat16)


def kernel(
    sizes, geno, pheno, perms, starts, maxima, moments, pooled,
    rows, table, base, best, mask, stats, sums,
    send, recv, pass_send, pass_recv, stat_send, stat_recv, sum_send, sum_recv,
):
    n_gene, n_var, n_perm = sizes
    n_block = n_var * n_perm
    chips = n_block // 2
    half = rows.shape[1]
    samples = rows.shape[2]
    width, genes = maxima.shape
    tiles, tile_cols, _ = table.shape
    per_tile = tile_cols // genes
    square = n_var == 4 and n_perm == 2

    gene_at = lax.axis_index("gene")
    var_at = lax.axis_index("var")
    perm_at = lax.axis_index("perm")
    core = lax.rem(var_at, 2)
    chip = (var_at // 2) * n_perm + perm_at
    me = var_at * n_perm + perm_at

    def device_of(chip_at, core_at):
        return {"var": (chip_at // n_perm) * 2 + core_at, "perm": lax.rem(chip_at, n_perm)}

    def block_of(chip_at, core_at):
        return ((chip_at // n_perm) * 2 + core_at) * n_perm + lax.rem(chip_at, n_perm)

    def block_peer(step):
        other = lax.rem(me + step, n_block)
        return {"var": other // n_perm, "perm": lax.rem(other, n_perm)}

    def gene_peer(step):
        return {"gene": lax.rem(gene_at + step, n_gene)}

    barrier = pltpu.get_barrier_semaphore()
    for step in range(1, n_block):
        pl.semaphore_signal(barrier, inc=1, device_id=block_peer(step), device_id_type=MESH)
    for step in range(1, n_gene):
        pl.semaphore_signal(barrier, inc=1, device_id=gene_peer(step), device_id_type=MESH)

    for part in range(2):
        rows[me * 2 + part] = standard_rows(geno[pl.ds(part * half, half), :])
    base[...] = standard_rows(pheno[...])
    best[...] = jnp.zeros_like(best)
    pl.semaphore_wait(barrier, n_block - 1 + n_gene - 1)

    def shift(step, back=False):
        if square:
            flip_y, flip_x = step // 2, step % 2
            y, x = chip // 2, lax.rem(chip, 2)
            y = 1 - y if flip_y else y
            x = 1 - x if flip_x else x
            return y * 2 + x
        return lax.rem(chip + (chips - step if back else step), chips)

    waiting = []

    def start(chunk, target, send_sem, recv_sem):
        copy = pltpu.make_async_remote_copy(
            src_ref=rows.at[chunk], dst_ref=rows.at[chunk], send_sem=send_sem,
            recv_sem=recv_sem, device_id=target, device_id_type=MESH,
        )
        copy.start()
        waiting.append(copy)

    def arrive(chunk, recv_sem):
        pltpu.make_async_remote_copy(
            src_ref=rows.at[chunk], dst_ref=rows.at[chunk], send_sem=send.at[0, 0],
            recv_sem=recv_sem, device_id=partner, device_id_type=MESH,
        ).wait_recv()

    partner = device_of(chip, 1 - core)

    def to_chip(step, part):
        start(me * 2 + part, device_of(shift(step), core), send.at[step, part], recv.at[step, part])

    def to_partner(chunk, step, part):
        start(chunk, partner, pass_send.at[step, part], pass_recv.at[step, part])

    if square:
        to_chip(1, 0)
        to_chip(2, 1)
        to_partner(me * 2, 0, 0)
        to_partner(me * 2 + 1, 0, 1)
        to_chip(1, 1)
        to_chip(2, 0)
    else:
        to_partner(me * 2, 0, 0)
        to_partner(me * 2 + 1, 0, 1)
        for step in range(1, chips):
            for part in range(2):
                to_chip(step, part)

    def build(at, carry):
        for pair in range(per_tile):
            order = perms[pl.ds(at * per_tile + pair, 1), :]
            picked = lax.broadcasted_iota(jnp.int32, (samples, samples), 0) == order
            select = jnp.where(picked, 1.0, 0.0).astype(jnp.bfloat16)
            placed = jnp.dot(base[...], select, preferred_element_type=jnp.float32)
            table[at, pl.ds(pair * genes, genes), :] = placed.astype(jnp.bfloat16)
        return carry

    lax.fori_loop(0, tiles, build, 0)

    unroll = min(UNROLL, tiles)

    def score(chunks):
        def one_chunk(at, carry):
            chunk = chunks[0]
            for place in range(1, len(chunks)):
                chunk = jnp.where(at == place, chunks[place], chunk)
            row = chunk * half + lax.broadcasted_iota(jnp.int32, (half, genes), 0)
            first = starts[...]
            mask[...] = jnp.where((row >= first) & (row < first + WINDOW), 1.0, 0.0)

            def some_tiles(group, inner):
                for place in range(unroll):
                    tile = group * unroll + place
                    found = lax.dot_general(
                        rows[chunk], table[tile], (((1,), (1,)), ((), ())),
                        preferred_element_type=jnp.float32,
                    )
                    for pair in range(per_tile):
                        part = found[:, pair * genes:(pair + 1) * genes]
                        part = part * part * mask[...]
                        top = jnp.max(part.reshape(half // 8, 8, genes), axis=0)
                        slot = tile * per_tile + pair
                        best[slot] = jnp.maximum(best[slot], top)
                return inner

            return lax.fori_loop(0, tiles // unroll, some_tiles, carry)

        lax.fori_loop(0, len(chunks), one_chunk, 0)

    def chunk_at(step, core_at, part):
        return block_of(shift(step, back=True) if step else chip, core_at) * 2 + part

    def stage(arrivals, relay):
        if arrivals[0][0]:
            for step, part in arrivals:
                chunk = chunk_at(step, core, part)
                arrive(chunk, recv.at[step, part])
                if relay:
                    other = 3 - step
                    start(chunk, device_of(shift(other), core), send.at[3, part], recv.at[3, part])
                to_partner(chunk, step, part)
        score([chunk_at(step, core, part) for step, part in arrivals])
        for step, part in arrivals:
            arrive(chunk_at(step, 1 - core, part), pass_recv.at[step, part])
        score([chunk_at(step, 1 - core, part) for step, part in arrivals])

    stage([(0, 0), (0, 1)], False)
    if square:
        stage([(1, 0), (2, 1)], True)
        stage([(1, 1), (2, 0)], False)
        stage([(3, 0), (3, 1)], False)
    else:
        for step in range(1, chips):
            stage([(step, 0), (step, 1)], False)

    top = jnp.max(best[...], axis=1) * samples
    maxima[...] = top
    log_stat = jnp.log1p(top)
    total = jnp.sum(log_stat, axis=0, keepdims=True)
    total_sq = jnp.sum(log_stat * log_stat, axis=0, keepdims=True)
    line = lax.broadcasted_iota(jnp.int32, (8, genes), 0)
    stats[me] = jnp.where(line == 0, total, jnp.where(line == 1, total_sq, 0.0))
    exchange = []
    for step in range(1, n_block):
        copy = pltpu.make_async_remote_copy(
            src_ref=stats.at[me], dst_ref=stats.at[me], send_sem=stat_send.at[step],
            recv_sem=stat_recv.at[step], device_id=block_peer(step), device_id_type=MESH,
        )
        copy.start()
        exchange.append(copy)
    for step, copy in enumerate(exchange, 1):
        other = lax.rem(me + n_block - step, n_block)
        pltpu.make_async_remote_copy(
            src_ref=stats.at[other], dst_ref=stats.at[other], send_sem=stat_send.at[step],
            recv_sem=stat_recv.at[step], device_id=partner, device_id_type=MESH,
        ).wait_recv()
    mean = jnp.sum(stats[...], axis=0) / (width * n_block)
    moments[...] = mean[0:2, :]
    sums[gene_at] = mean
    for step in range(1, n_gene):
        copy = pltpu.make_async_remote_copy(
            src_ref=sums.at[gene_at], dst_ref=sums.at[gene_at], send_sem=sum_send.at[step],
            recv_sem=sum_recv.at[step], device_id=gene_peer(step), device_id_type=MESH,
        )
        copy.start()
        exchange.append(copy)
    for step in range(1, n_gene):
        other = lax.rem(gene_at + n_gene - step, n_gene)
        pltpu.make_async_remote_copy(
            src_ref=sums.at[other], dst_ref=sums.at[other], send_sem=sum_send.at[step],
            recv_sem=sum_recv.at[step], device_id=partner, device_id_type=MESH,
        ).wait_recv()
    whole = jnp.sum(sums[...], axis=0)
    pooled[...] = jnp.sum(whole, axis=1, keepdims=True)[0:2, :] / (genes * n_gene)
    for copy in waiting + exchange:
        copy.wait_send()


def solution(mesh):
    n_gene, n_var, n_perm = (mesh.shape[name] for name in ("gene", "var", "perm"))
    n_block = n_var * n_perm

    def shards(genotypes, phenotypes, perm_rows, starts):
        _, local_rows, samples = genotypes.shape
        genes = phenotypes.shape[0]
        width = perm_rows.shape[0]
        half = local_rows // 2
        per_tile = max(256 // genes, 1)
        tiles = width // per_tile
        chips = n_block // 2
        steps = max(chips, 4)
        dma = pltpu.SemaphoreType.DMA
        vmem = pl.BlockSpec(memory_space=pltpu.VMEM)
        flops = 2 * width * genes * samples * (local_rows * n_block + samples)
        maxima, moments, pooled = pl.pallas_call(
            functools.partial(kernel, (n_gene, n_var, n_perm)),
            out_shape=(
                jax.ShapeDtypeStruct((width, genes), jnp.float32),
                jax.ShapeDtypeStruct((2, genes), jnp.float32),
                jax.ShapeDtypeStruct((2, 1), jnp.float32),
            ),
            in_specs=[vmem] * 4,
            out_specs=(vmem,) * 3,
            scratch_shapes=[
                pltpu.VMEM((n_block * 2, half, samples), jnp.bfloat16),
                pltpu.VMEM((tiles, per_tile * genes, samples), jnp.bfloat16),
                pltpu.VMEM((genes, samples), jnp.bfloat16),
                pltpu.VMEM((width, 8, genes), jnp.float32),
                pltpu.VMEM((half, genes), jnp.float32),
                pltpu.VMEM((n_block, 8, genes), jnp.float32),
                pltpu.VMEM((n_gene, 8, genes), jnp.float32),
                dma((steps, 2)), dma((steps, 2)), dma((steps, 2)), dma((steps, 2)),
                dma((n_block,)), dma((n_block,)), dma((n_gene,)), dma((n_gene,)),
            ],
            compiler_params=pltpu.CompilerParams(
                collective_id=0, has_side_effects=True, vmem_limit_bytes=56 * 1024 * 1024
            ),
            cost_estimate=pl.CostEstimate(
                flops=flops, bytes_accessed=local_rows * samples * 2, transcendentals=0
            ),
        )(genotypes[0], phenotypes, perm_rows, starts.reshape(1, genes))
        return maxima, moments, pooled.reshape(2)

    return jax.shard_map(
        shards,
        mesh=mesh,
        in_specs=(
            P("gene", ("var", "perm"), None),
            P("gene", None),
            P(("var", "perm"), None),
            P("gene"),
        ),
        out_specs=(P(("var", "perm"), "gene"), P(None, "gene"), P()),
        check_vma=False,
    )
```

```python
import functools

import jax
import jax.numpy as jnp
from jax import lax
from jax.experimental import pallas as pl
from jax.experimental.pallas import tpu as pltpu
from jax.sharding import PartitionSpec as P

WINDOW = 4096
MESH = pl.DeviceIdType.MESH
UNROLL = 8


def standard_rows(values):
    as_float = values.astype(jnp.float32)
    centred = as_float - jnp.mean(as_float, axis=1, keepdims=True)
    inv_norm = lax.rsqrt(jnp.sum(centred * centred, axis=1, keepdims=True) + 1.0)
    return (centred * inv_norm).astype(jnp.bfloat16)


def kernel(
    sizes, geno, pheno, perms, starts, packed,
    rows, table, base, best, mask, stats, sums,
    send, recv, pass_send, pass_recv, far_send, far_recv, far_pass_send, far_pass_recv,
    stat_send, stat_recv, sum_send, sum_recv,
):
    n_gene, n_var, n_perm = sizes
    n_block = n_var * n_perm
    chips = n_block // 2
    quarter = rows.shape[1]
    half = 2 * quarter
    samples = rows.shape[2]
    width, genes = perms.shape[0], packed.shape[1]
    tiles, tile_cols, _ = table.shape
    per_tile = tile_cols // genes
    square = n_var == 4 and n_perm == 2

    gene_at = lax.axis_index("gene")
    var_at = lax.axis_index("var")
    perm_at = lax.axis_index("perm")
    core = lax.rem(var_at, 2)
    chip = (var_at // 2) * n_perm + perm_at
    me = var_at * n_perm + perm_at

    def device_of(chip_at, core_at):
        return {"var": (chip_at // n_perm) * 2 + core_at, "perm": lax.rem(chip_at, n_perm)}

    def block_of(chip_at, core_at):
        return ((chip_at // n_perm) * 2 + core_at) * n_perm + lax.rem(chip_at, n_perm)

    def block_peer(step):
        other = lax.rem(me + step, n_block)
        return {"var": other // n_perm, "perm": lax.rem(other, n_perm)}

    def gene_peer(step):
        return {"gene": lax.rem(gene_at + step, n_gene)}

    barrier = pltpu.get_barrier_semaphore()
    for step in range(1, n_block):
        pl.semaphore_signal(barrier, inc=1, device_id=block_peer(step), device_id_type=MESH)
    for step in range(1, n_gene):
        pl.semaphore_signal(barrier, inc=1, device_id=gene_peer(step), device_id_type=MESH)

    for part in range(2):
        ready = standard_rows(geno[pl.ds(part * half, half), :])
        rows[me * 4 + part * 2] = ready[:quarter]
        rows[me * 4 + part * 2 + 1] = ready[quarter:]
    base[...] = standard_rows(pheno[...])
    best[...] = jnp.zeros_like(best)
    pl.semaphore_wait(barrier, n_block - 1 + n_gene - 1)

    def shift(step, back=False):
        if square:
            flip_y, flip_x = step // 2, step % 2
            y, x = chip // 2, lax.rem(chip, 2)
            y = 1 - y if flip_y else y
            x = 1 - x if flip_x else x
            return y * 2 + x
        return lax.rem(chip + (chips - step if back else step), chips)

    waiting = []

    def start(chunk, count, target, send_sem, recv_sem):
        piece = rows.at[pl.ds(chunk, count)]
        copy = pltpu.make_async_remote_copy(
            src_ref=piece, dst_ref=piece, send_sem=send_sem,
            recv_sem=recv_sem, device_id=target, device_id_type=MESH,
        )
        copy.start()
        waiting.append(copy)

    def arrive(chunk, count, recv_sem):
        piece = rows.at[pl.ds(chunk, count)]
        pltpu.make_async_remote_copy(
            src_ref=piece, dst_ref=piece, send_sem=send.at[0, 0],
            recv_sem=recv_sem, device_id=partner, device_id_type=MESH,
        ).wait_recv()

    partner = device_of(chip, 1 - core)

    def to_chip(step, part):
        start(
            me * 4 + part * 2, 2, device_of(shift(step), core),
            send.at[step, part], recv.at[step, part],
        )

    def to_partner(chunk, step, part):
        start(chunk, 2, partner, pass_send.at[step, part], pass_recv.at[step, part])

    if square:
        to_chip(1, 0)
        to_chip(2, 1)
        to_partner(me * 4, 0, 0)
        to_partner(me * 4 + 2, 0, 1)
        to_chip(1, 1)
        to_chip(2, 0)
    else:
        to_partner(me * 4, 0, 0)
        to_partner(me * 4 + 2, 0, 1)
        for step in range(1, chips):
            for part in range(2):
                to_chip(step, part)

    def build(at, carry):
        for pair in range(per_tile):
            order = perms[pl.ds(at * per_tile + pair, 1), :]
            picked = lax.broadcasted_iota(jnp.int32, (samples, samples), 0) == order
            select = jnp.where(picked, 1.0, 0.0).astype(jnp.bfloat16)
            placed = jnp.dot(base[...], select, preferred_element_type=jnp.float32)
            table[at, pl.ds(pair * genes, genes), :] = placed.astype(jnp.bfloat16)
        return carry

    lax.fori_loop(0, tiles, build, 0)

    unroll = min(UNROLL, tiles)

    def score(chunks):
        def one_chunk(at, carry):
            pieces = chunks[0]
            for place in range(1, len(chunks)):
                pieces = [jnp.where(at == place, new, old) for new, old in zip(chunks[place], pieces)]
            first = starts[...]
            for place, piece in enumerate(pieces):
                row = piece * quarter + lax.broadcasted_iota(jnp.int32, (quarter, genes), 0)
                inside = (row >= first) & (row < first + WINDOW)
                mask[pl.ds(place * quarter, quarter), :] = jnp.where(inside, 1.0, 0.0)

            def some_tiles(group, inner):
                for place in range(unroll):
                    tile = group * unroll + place
                    found = lax.dot_general(
                        jnp.concatenate([rows[piece] for piece in pieces], axis=0), table[tile], (((1,), (1,)), ((), ())),
                        preferred_element_type=jnp.float32,
                    )
                    for pair in range(per_tile):
                        part = found[:, pair * genes:(pair + 1) * genes]
                        part = part * part * mask[...]
                        top = jnp.max(part.reshape(half // 8, 8, genes), axis=0)
                        slot = tile * per_tile + pair
                        best[slot] = jnp.maximum(best[slot], top)
                return inner

            return lax.fori_loop(0, tiles // unroll, some_tiles, carry)

        lax.fori_loop(0, len(chunks), one_chunk, 0)

    def chunk_at(step, core_at, part):
        return block_of(shift(step, back=True) if step else chip, core_at) * 4 + part * 2

    def halves(arrivals, core_at):
        found = [chunk_at(step, core_at, part) for step, part in arrivals]
        return [(chunk, chunk + 1) for chunk in found]

    def stage(arrivals, relay):
        if arrivals[0][0]:
            for step, part in arrivals:
                chunk = chunk_at(step, core, part)
                arrive(chunk, 2, recv.at[step, part])
                if relay:
                    target = device_of(shift(3 - step), core)
                    for piece in range(2):
                        start(
                            chunk + piece, 1, target,
                            far_send.at[part, piece], far_recv.at[part, piece],
                        )
                to_partner(chunk, step, part)
        score(halves(arrivals, core))
        for step, part in arrivals:
            arrive(chunk_at(step, 1 - core, part), 2, pass_recv.at[step, part])
        score(halves(arrivals, 1 - core))

    def far_stage(piece):
        own = [chunk_at(3, core, part) + piece for part in range(2)]
        passed = [chunk_at(3, 1 - core, part) + piece for part in range(2)]
        for part in range(2):
            arrive(own[part], 1, far_recv.at[part, piece])
            start(
                own[part], 1, partner,
                far_pass_send.at[part, piece], far_pass_recv.at[part, piece],
            )
        score([own])
        for part in range(2):
            arrive(passed[part], 1, far_pass_recv.at[part, piece])
        score([passed])

    stage([(0, 0), (0, 1)], False)
    if square:
        stage([(1, 0), (2, 1)], True)
        stage([(1, 1), (2, 0)], False)
        far_stage(0)
        far_stage(1)
    else:
        for step in range(1, chips):
            stage([(step, 0), (step, 1)], False)

    top = jnp.max(best[...], axis=1) * samples
    packed[pl.ds(0, width), :] = top
    log_stat = jnp.log1p(top)
    total = jnp.sum(log_stat, axis=0, keepdims=True)
    total_sq = jnp.sum(log_stat * log_stat, axis=0, keepdims=True)
    line = lax.broadcasted_iota(jnp.int32, (8, genes), 0)
    stats[me] = jnp.where(line == 0, total, jnp.where(line == 1, total_sq, 0.0))
    exchange = []
    for step in range(1, n_block):
        copy = pltpu.make_async_remote_copy(
            src_ref=stats.at[me], dst_ref=stats.at[me], send_sem=stat_send.at[step],
            recv_sem=stat_recv.at[step], device_id=block_peer(step), device_id_type=MESH,
        )
        copy.start()
        exchange.append(copy)
    for step, copy in enumerate(exchange, 1):
        other = lax.rem(me + n_block - step, n_block)
        pltpu.make_async_remote_copy(
            src_ref=stats.at[other], dst_ref=stats.at[other], send_sem=stat_send.at[step],
            recv_sem=stat_recv.at[step], device_id=partner, device_id_type=MESH,
        ).wait_recv()
    mean = jnp.sum(stats[...], axis=0) / (width * n_block)
    sums[gene_at] = mean
    for step in range(1, n_gene):
        copy = pltpu.make_async_remote_copy(
            src_ref=sums.at[gene_at], dst_ref=sums.at[gene_at], send_sem=sum_send.at[step],
            recv_sem=sum_recv.at[step], device_id=gene_peer(step), device_id_type=MESH,
        )
        copy.start()
        exchange.append(copy)
    for step in range(1, n_gene):
        other = lax.rem(gene_at + n_gene - step, n_gene)
        pltpu.make_async_remote_copy(
            src_ref=sums.at[other], dst_ref=sums.at[other], send_sem=sum_send.at[step],
            recv_sem=sum_recv.at[step], device_id=partner, device_id_type=MESH,
        ).wait_recv()
    whole = jnp.sum(sums[...], axis=0)
    overall = jnp.sum(whole, axis=1, keepdims=True) / (genes * n_gene)
    spread = pltpu.roll(jnp.broadcast_to(overall, (8, genes)), 2, 0)
    packed[pl.ds(width, 8), :] = jnp.where(line < 2, mean, spread)
    for copy in waiting + exchange:
        copy.wait_send()


def unpack(packed, maxima, moments, pooled):
    width = maxima.shape[0]
    maxima[...] = packed[pl.ds(0, width), :]
    moments[...] = packed[pl.ds(width, 2), :]
    for place in range(2):
        pooled[place] = packed[width + 2 + place, 0]


def solution(mesh):
    n_gene, n_var, n_perm = (mesh.shape[name] for name in ("gene", "var", "perm"))
    n_block = n_var * n_perm

    def shards(genotypes, phenotypes, perm_rows, starts):
        _, local_rows, samples = genotypes.shape
        genes = phenotypes.shape[0]
        width = perm_rows.shape[0]
        quarter = local_rows // 4
        per_tile = max(256 // genes, 1)
        tiles = width // per_tile
        chips = n_block // 2
        steps = max(chips, 4)
        dma = pltpu.SemaphoreType.DMA
        vmem = pl.BlockSpec(memory_space=pltpu.VMEM)
        flops = 2 * width * genes * samples * (local_rows * n_block + samples)
        packed = pl.pallas_call(
            functools.partial(kernel, (n_gene, n_var, n_perm)),
            out_shape=jax.ShapeDtypeStruct((width + 8, genes), jnp.float32),
            in_specs=[vmem] * 4,
            out_specs=vmem,
            scratch_shapes=[
                pltpu.VMEM((n_block * 4, quarter, samples), jnp.bfloat16),
                pltpu.VMEM((tiles, per_tile * genes, samples), jnp.bfloat16),
                pltpu.VMEM((genes, samples), jnp.bfloat16),
                pltpu.VMEM((width, 8, genes), jnp.float32),
                pltpu.VMEM((2 * quarter, genes), jnp.float32),
                pltpu.VMEM((n_block, 8, genes), jnp.float32),
                pltpu.VMEM((n_gene, 8, genes), jnp.float32),
                dma((steps, 2)), dma((steps, 2)), dma((steps, 2)), dma((steps, 2)),
                dma((2, 2)), dma((2, 2)), dma((2, 2)), dma((2, 2)),
                dma((n_block,)), dma((n_block,)), dma((n_gene,)), dma((n_gene,)),
            ],
            compiler_params=pltpu.CompilerParams(
                collective_id=0, has_side_effects=True, vmem_limit_bytes=56 * 1024 * 1024
            ),
            cost_estimate=pl.CostEstimate(
                flops=flops, bytes_accessed=local_rows * samples * 2, transcendentals=0
            ),
        )(genotypes[0], phenotypes, perm_rows, starts.reshape(1, genes))
        return pl.pallas_call(
            unpack,
            out_shape=(
                jax.ShapeDtypeStruct((width, genes), jnp.float32),
                jax.ShapeDtypeStruct((2, genes), jnp.float32),
                jax.ShapeDtypeStruct((2,), jnp.float32),
            ),
            in_specs=[vmem],
            out_specs=(vmem, vmem, pl.BlockSpec(memory_space=pltpu.SMEM)),
        )(packed)

    return jax.shard_map(
        shards,
        mesh=mesh,
        in_specs=(
            P("gene", ("var", "perm"), None),
            P("gene", None),
            P(("var", "perm"), None),
            P("gene"),
        ),
        out_specs=(P(("var", "perm"), "gene"), P(None, "gene"), P()),
        check_vma=False,
    )
```
